32 devices in a mesh: groups: 2 (over y), grid: 4 (over z), depth: 4 (over x, core).
Axes of the slice: x: 2, y: 2, z: 4, core: 2. Of those that a mesh axis runs over, the one named last changes fastest.
Arguments:
- tokens: bfloat16 [512, 4096], P(('groups', 'grid'), 'depth'), parts along dimension 0, may hold values from -6 to 6
- gate_weight: bfloat16 [4096, 14336], P('depth', 'grid'), may hold values from -0.09375 to 0.09375
- up_weight: bfloat16 [4096, 14336], P('depth', 'grid'), may hold values from -0.09375 to 0.09375
- down_weight: bfloat16 [14336, 4096], P('grid', 'depth'), may hold values from -0.046875 to 0.046875
Outputs:
- mixed: bfloat16 [512, 4096], P(('groups', 'grid'), 'depth'), parts along dimension 0
The draws below stay inside these ranges and needn't reach their ends.
There are 2 independent parts, one for each index of `groups`. The reference program is written for one: setup_inputs(seed, part) draws one part's arguments, and reference() takes and returns one part's arrays. A program takes and returns all parts, laid end to end along the dimension named above; an argument that names none is the same for every part. Nothing has to cross between parts.
All inputs are finite; a program needn't handle non-finite values.
Results may differ from the reference program's by a relative error of at most 0.0049.
Values may be sent and summed in bfloat16 or wider, within the bound.
No kernel may reach another device: no remote copies, remote signals or barrier semaphores. Data moves between devices by JAX's collectives and lax.ppermute only.
A program may use at most 64 MiB of HBM per device.

```python
import jax
import jax.numpy as jnp

D = 4096
FF = 14336
TOK = 256


def steps_of(rng, extent, pieces, low, largest):
    loudness, own = 1.0, jax.random.fold_in(rng, 6)
    for axis_at, shards_of in pieces:
        draws = jnp.exp(jax.random.uniform(jax.random.fold_in(own, axis_at), (shards_of,), jnp.float32, low / len(pieces), largest / len(pieces)))
        loudness = loudness * jnp.repeat(draws, extent[axis_at] // shards_of).reshape([-1 if axis == axis_at else 1 for axis in range(len(extent))])
    return loudness


def noise(stream_key, dims, spread, limit, split=(), kind=jnp.bfloat16):
    entries = jax.random.normal(stream_key, dims, jnp.float32) * spread
    if len(split) > 0:
        entries = steps_of(stream_key, dims, split, -0.22, 0.18) * entries
    return jnp.clip(entries, min=-limit, max=limit).astype(kind)


def setup_inputs(seed: int = 0, part: int = 0) -> dict:
    keys = jax.random.split(jax.random.key(seed), 5)
    own_keys = jax.random.split(jax.random.fold_in(keys[4], part), 5)
    return {
        "tokens": noise(own_keys[0], (TOK, D), 1.0, 6.0, ((0, 4), (1, 4))),
        "gate_weight": noise(keys[1], (D, FF), D ** -0.5, 0.09375, ((0, 4), (1, 4))),
        "up_weight": noise(keys[2], (D, FF), D ** -0.5, 0.09375, ((0, 4), (1, 4))),
        "down_weight": noise(keys[3], (FF, D), FF ** -0.5, 0.046875, ((0, 4), (1, 4))),
    }


def reference(tokens, gate_weight, up_weight, down_weight):
    gate = jnp.dot(tokens, gate_weight, preferred_element_type=jnp.float32)
    up = jnp.dot(tokens, up_weight, preferred_element_type=jnp.float32)
    hidden = (jax.nn.silu(gate) * up).astype(jnp.bfloat16)
    return jnp.dot(hidden, down_weight, preferred_element_type=jnp.float32).astype(jnp.bfloat16)
```

```python
import functools

import jax
import jax.numpy as jnp
from jax import lax
from jax.experimental import pallas as pl
from jax.experimental.pallas import tpu as pltpu
from jax.sharding import PartitionSpec as P


CHUNKS = ((0,), (1,), (3,), (2,))
ORDER = (3, 1, 2, 0)
MIB = 1024 * 1024
VMEM = pl.BlockSpec(memory_space=pltpu.VMEM)
SMEM = pl.BlockSpec(memory_space=pltpu.SMEM)


def flip(value, axis, bits):
    size = lax.axis_size(axis)
    return lax.ppermute(value, axis, [(i, i ^ bits) for i in range(size)])


def held(value):
    return pltpu.with_memory_space_constraint(value, pltpu.VMEM)


def width_of(hidden):
    return next((w for w in (896, 512, 384, 256, 128) if hidden % w == 0), hidden)


def sort_rows(me, x_refs, x_sc):
    blocks, part = len(x_refs), x_refs[0].shape[0] // len(ORDER)
    for i, r in enumerate(ORDER):
        at = pl.multiple_of((me ^ r) * part, part)
        for b in range(blocks):
            x_sc[(i * blocks + b) * part : (i * blocks + b + 1) * part, :] = x_refs[b][pl.ds(at, part), :]


def sort_kernel(me_ref, *refs):
    sort_rows(me_ref[0], refs[:-1], refs[-1])


def sort(me, xs):
    block_rows, depth = xs[0].shape
    return pl.pallas_call(
        sort_kernel,
        in_specs=[SMEM] + [VMEM] * len(xs),
        out_specs=VMEM,
        out_shape=jax.ShapeDtypeStruct((block_rows * len(xs), depth), xs[0].dtype),
        compiler_params=pltpu.CompilerParams(vmem_limit_bytes=12 * MIB),
        cost_estimate=pl.CostEstimate(flops=10**10, bytes_accessed=0, transcendentals=0),
        name="sort",
    )(me, *xs)


def up_gate_kernel(me_ref, *refs, blocks):
    x_refs, (g_ref, u_ref, send_ref, keep_ref, *scratch) = refs[:blocks], refs[blocks:]
    if scratch:
        sort_rows(me_ref[0], x_refs, scratch[0])
    x = (scratch or x_refs)[0][...]
    half = x.shape[0] // 2
    hidden = g_ref.shape[1]
    width = width_of(hidden)
    for j in range(hidden // width):
        cols = slice(j * width, (j + 1) * width)
        for i, w_ref in enumerate((g_ref, u_ref)):
            y = jnp.dot(x, w_ref[:, cols], preferred_element_type=jnp.float32)
            send_ref[i, :, cols] = y[:half].astype(send_ref.dtype)
            keep_ref[i, :, cols] = y[half:]


def up_gate(me, xs, gate, up, ordered):
    depth, hidden = gate.shape
    rows = xs[0].shape[0] * len(xs)
    return pl.pallas_call(
        functools.partial(up_gate_kernel, blocks=len(xs)),
        in_specs=[SMEM] + [VMEM] * (len(xs) + 2),
        out_specs=[VMEM] * 2,
        out_shape=[
            jax.ShapeDtypeStruct((2, rows // 2, hidden), jnp.bfloat16),
            jax.ShapeDtypeStruct((2, rows // 2, hidden), jnp.float32),
        ],
        scratch_shapes=[] if ordered else [pltpu.VMEM((rows, depth), jnp.bfloat16)],
        compiler_params=pltpu.CompilerParams(vmem_limit_bytes=12 * MIB),
        cost_estimate=pl.CostEstimate(
            flops=4 * rows * depth * hidden, bytes_accessed=4 * depth * hidden, transcendentals=0
        ),
        name="up_gate",
    )(me, *xs, held(gate), held(up))


def down_kernel(me_ref, h0, h2, h1, h3, w_ref, *outs):
    me = me_ref[0]
    h = jnp.concatenate([h0[...], h2[...], h1[...], h3[...]], axis=0)
    part = outs[0].shape[0] // len(ORDER)
    depth = w_ref.shape[1]
    width = 256 if depth % 256 == 0 else depth
    for c in range(depth // width):
        cols = slice(c * width, (c + 1) * width)
        y = jnp.dot(h, w_ref[:, cols], preferred_element_type=jnp.float32)
        for i, r in enumerate((0, 2, 1, 3)):
            at = pl.multiple_of((me ^ r) * part, part)
            for b, out in enumerate(outs):
                first = (i * len(outs) + b) * part
                out[pl.ds(at, part), cols] = y[first : first + part].astype(out.dtype)


def down(me, hs, weight, block_rows, kinds):
    hidden, depth = weight.shape
    rows = block_rows * len(kinds)
    return pl.pallas_call(
        down_kernel,
        in_specs=[SMEM] + [VMEM] * 5,
        out_specs=[VMEM] * len(kinds),
        out_shape=[jax.ShapeDtypeStruct((block_rows, depth), kind) for kind in kinds],
        compiler_params=pltpu.CompilerParams(vmem_limit_bytes=12 * MIB),
        cost_estimate=pl.CostEstimate(
            flops=2 * rows * depth * hidden, bytes_accessed=2 * depth * hidden, transcendentals=0
        ),
        name="down",
    )(me, *hs, held(weight))


def steps(tokens, gate_weight, up_weight, down_weight):
    grid_size = lax.axis_size("grid")
    block_rows = tokens.shape[0]
    me = lax.axis_index("depth").astype(jnp.int32).reshape(1)
    per = grid_size // sum(map(len, CHUNKS))
    chunks = [[s for q in chunk for s in range(q * per, (q + 1) * per)] for chunk in CHUNKS]
    blocks = {0: tokens}
    for chunk in chunks:
        for s in chunk:
            if s:
                blocks[s] = flip(tokens, "grid", s)
    total = None
    arrived = []
    for number, chunk in enumerate(chunks):
        xs = [blocks[s] for s in chunk]
        if number == 0:
            xs = [sort(me, xs)]
        send, keep = up_gate(me, xs, gate_weight, up_weight, number == 0)
        part = keep.shape[1] // 2
        recv = flip(send, "depth", 1)
        across = (keep[:, :part] + recv[:, :part].astype(jnp.float32)).astype(jnp.bfloat16)
        crossed = flip(across, "depth", 2)
        both = keep[:, part:] + recv[:, part:].astype(jnp.float32) + crossed.astype(jnp.float32)
        mine = (jax.nn.silu(both[0]) * both[1]).astype(jnp.bfloat16)
        other = flip(mine, "depth", 2)
        mine_passed = flip(mine, "depth", 1)
        other_passed = flip(other, "depth", 1)
        kinds = [jnp.bfloat16 if s else jnp.float32 for s in chunk]
        outs = down(me, (mine, other, mine_passed, other_passed), down_weight, block_rows, kinds)
        for s, out in zip(chunk, outs):
            if s:
                arrived.append(flip(out, "grid", s))
            else:
                total = out
    for value in arrived:
        total = total + value.astype(jnp.float32)
    return total.astype(jnp.bfloat16)


def solution(mesh):
    placed = (
        P(("groups", "grid"), "depth"),
        P("depth", "grid"),
        P("depth", "grid"),
        P("grid", "depth"),
    )
    return jax.shard_map(
        steps, mesh=mesh, in_specs=placed, out_specs=P(("groups", "grid"), "depth"), check_vma=False
    )
```

```python
import functools

import jax
import jax.numpy as jnp
from jax import lax
from jax.experimental import pallas as pl
from jax.experimental.pallas import tpu as pltpu
from jax.sharding import PartitionSpec as P


CHUNKS = ((0,), (1,), (3,), (2,))
FAR = 2
SPLIT = {0: 2}
ORDER = (3, 1, 2, 0)
MIB = 1024 * 1024
VMEM = pl.BlockSpec(memory_space=pltpu.VMEM)
SMEM = pl.BlockSpec(memory_space=pltpu.SMEM)


def flip(value, axis, bits):
    size = lax.axis_size(axis)
    return lax.ppermute(value, axis, [(i, i ^ bits) for i in range(size)])


def held(value):
    return pltpu.with_memory_space_constraint(value, pltpu.VMEM)


def width_of(hidden):
    return next((w for w in (896, 512, 384, 256, 128) if hidden % w == 0), hidden)


def sort_rows(me, x_refs, x_sc):
    blocks, part = len(x_refs), x_refs[0].shape[0] // len(ORDER)
    for i, r in enumerate(ORDER):
        at = pl.multiple_of((me ^ r) * part, part)
        for b in range(blocks):
            x_sc[(i * blocks + b) * part : (i * blocks + b + 1) * part, :] = x_refs[b][pl.ds(at, part), :]


def sort_kernel(me_ref, *refs):
    sort_rows(me_ref[0], refs[:-1], refs[-1])


def sort(me, xs):
    block_rows, depth = xs[0].shape
    return pl.pallas_call(
        sort_kernel,
        in_specs=[SMEM] + [VMEM] * len(xs),
        out_specs=VMEM,
        out_shape=jax.ShapeDtypeStruct((block_rows * len(xs), depth), xs[0].dtype),
        compiler_params=pltpu.CompilerParams(vmem_limit_bytes=12 * MIB),
        cost_estimate=pl.CostEstimate(flops=10**10, bytes_accessed=0, transcendentals=0),
        name="sort",
    )(me, *[pltpu.with_memory_space_constraint(x, pltpu.HBM) for x in xs])


def up_gate_kernel(me_ref, *refs, blocks, first):
    x_refs, (g_ref, u_ref, send_ref, keep_ref, *scratch) = refs[:blocks], refs[blocks:]
    if scratch:
        sort_rows(me_ref[0], x_refs, scratch[0])
    x = (scratch or x_refs)[0][...]
    half = x.shape[0] // 2
    share = send_ref.shape[2]
    width = width_of(share)
    for j in range(share // width):
        cols = slice(j * width, (j + 1) * width)
        taken = slice(first + j * width, first + (j + 1) * width)
        for i, w_ref in enumerate((g_ref, u_ref)):
            y = jnp.dot(x, w_ref[:, taken], preferred_element_type=jnp.float32)
            send_ref[i, :, cols] = y[:half].astype(send_ref.dtype)
            keep_ref[i, :, cols] = y[half:]


def up_gate(me, xs, gate, up, ordered, piece, pieces):
    depth, hidden = gate.shape[0], gate.shape[1] // pieces
    rows = xs[0].shape[0] * len(xs)
    return pl.pallas_call(
        functools.partial(up_gate_kernel, blocks=len(xs), first=piece * hidden),
        in_specs=[SMEM] + [VMEM] * (len(xs) + 2),
        out_specs=[VMEM] * 2,
        out_shape=[
            jax.ShapeDtypeStruct((2, rows // 2, hidden), jnp.bfloat16),
            jax.ShapeDtypeStruct((2, rows // 2, hidden), jnp.float32),
        ],
        scratch_shapes=[] if ordered else [pltpu.VMEM((rows, depth), jnp.bfloat16)],
        compiler_params=pltpu.CompilerParams(vmem_limit_bytes=12 * MIB),
        cost_estimate=pl.CostEstimate(
            flops=4 * rows * depth * hidden, bytes_accessed=4 * depth * hidden, transcendentals=0
        ),
        name="up_gate",
    )(me, *xs, held(gate), held(up))


def down_kernel(me_ref, h0, h2, h1, h3, w_ref, *refs, blocks):
    outs, adds = refs[-blocks:], refs[:-blocks]
    me = me_ref[0]
    h = jnp.concatenate([h0[...], h2[...], h1[...], h3[...]], axis=0)
    part = outs[0].shape[0] // len(ORDER)
    depth = w_ref.shape[1]
    width = 256 if depth % 256 == 0 else depth
    for c in range(depth // width):
        cols = slice(c * width, (c + 1) * width)
        y = jnp.dot(h, w_ref[:, cols], preferred_element_type=jnp.float32)
        for i, r in enumerate((0, 2, 1, 3)):
            at = pl.multiple_of((me ^ r) * part, part)
            for b, out in enumerate(outs):
                first = (i * len(outs) + b) * part
                value = y[first : first + part]
                if adds:
                    value += adds[b][pl.ds(at, part), cols].astype(jnp.float32)
                out[pl.ds(at, part), cols] = value.astype(out.dtype)


def down(me, hs, weight, block_rows, kinds, adds):
    hidden, depth = weight.shape
    rows = block_rows * len(kinds)
    return pl.pallas_call(
        functools.partial(down_kernel, blocks=len(kinds)),
        in_specs=[SMEM] + [VMEM] * (5 + len(adds)),
        out_specs=[VMEM] * len(kinds),
        out_shape=[jax.ShapeDtypeStruct((block_rows, depth), kind) for kind in kinds],
        compiler_params=pltpu.CompilerParams(vmem_limit_bytes=12 * MIB),
        cost_estimate=pl.CostEstimate(
            flops=2 * rows * depth * hidden, bytes_accessed=2 * depth * hidden, transcendentals=0
        ),
        name="down",
    )(me, *hs, held(weight), *adds)


def steps(tokens, gate_weight, up_weight, down_weight):
    grid_size = lax.axis_size("grid")
    block_rows = tokens.shape[0]
    me = lax.axis_index("depth").astype(jnp.int32).reshape(1)
    per = grid_size // sum(map(len, CHUNKS))
    chunks = [[s for q in chunk for s in range(q * per, (q + 1) * per)] for chunk in CHUNKS]
    blocks = {0: tokens}
    for chunk in chunks:
        for s in chunk:
            if s:
                blocks[s] = flip(tokens, "grid", s)
    total = None
    arrived, relayed = [], {}
    for number, chunk in enumerate(chunks):
        xs = [blocks[s] for s in chunk]
        if number == 0:
            xs = [sort(me, xs)]
        pieces = SPLIT.get(number, 1) if gate_weight.shape[1] % 256 == 0 else 1
        sums = []
        for piece in range(pieces):
            send, keep = up_gate(me, xs, gate_weight, up_weight, number == 0, piece, pieces)
            part = keep.shape[1] // 2
            recv = flip(send, "depth", 1)
            across = (keep[:, :part] + recv[:, :part].astype(jnp.float32)).astype(jnp.bfloat16)
            crossed = flip(across, "depth", 2)
            sums.append((keep, recv, crossed))
        mine = []
        for keep, recv, crossed in sums:
            both = keep[:, part:] + recv[:, part:].astype(jnp.float32) + crossed.astype(jnp.float32)
            mine.append((jax.nn.silu(both[0]) * both[1]).astype(jnp.bfloat16))
        mine = jnp.concatenate(mine, axis=1)
        other = flip(mine, "depth", 2)
        mine_passed = flip(mine, "depth", 1)
        other_passed = flip(other, "depth", 1)
        kinds = [jnp.bfloat16 if s else jnp.float32 for s in chunk]
        adds = [relayed[s] for s in chunk if s in relayed]
        outs = down(me, (mine, other, mine_passed, other_passed), down_weight, block_rows, kinds, adds)
        for s, out in zip(chunk, outs):
            if s == 0:
                total = out
            else:
                if number == FAR:
                    relayed[s ^ per] = flip(out, "grid", per)
                else:
                    arrived.append(flip(out, "grid", s))
    for value in arrived:
        total = total + value.astype(jnp.float32)
    return total.astype(jnp.bfloat16)


def solution(mesh):
    placed = (
        P(("groups", "grid"), "depth"),
        P("depth", "grid"),
        P("depth", "grid"),
        P("grid", "depth"),
    )
    return jax.shard_map(
        steps, mesh=mesh, in_specs=placed, out_specs=P(("groups", "grid"), "depth"), check_vma=False
    )
```

```python
import functools

import jax
import jax.numpy as jnp
from jax import lax
from jax.experimental import pallas as pl
from jax.experimental.pallas import tpu as pltpu
from jax.sharding import PartitionSpec as P


CHUNKS = ((0,), (1,), (3,), (2,))
FAR = 2
SPLIT = {0: 2}
ORDER = (3, 1, 2, 0)
MIB = 1024 * 1024
VMEM = pl.BlockSpec(memory_space=pltpu.VMEM)
SMEM = pl.BlockSpec(memory_space=pltpu.SMEM)


def flip(value, axis, bits):
    size = lax.axis_size(axis)
    return lax.ppermute(value, axis, [(i, i ^ bits) for i in range(size)])


def held(value):
    return pltpu.with_memory_space_constraint(value, pltpu.VMEM)


def width_of(hidden):
    return next((w for w in (1792, 896, 512, 384, 256, 128) if hidden % w == 0), hidden)


def sort_rows(me, x_refs, x_sc):
    blocks, part = len(x_refs), x_refs[0].shape[0] // len(ORDER)
    for i, r in enumerate(ORDER):
        at = pl.multiple_of((me ^ r) * part, part)
        for b in range(blocks):
            x_sc[(i * blocks + b) * part : (i * blocks + b + 1) * part, :] = x_refs[b][pl.ds(at, part), :]


def sort_kernel(me_ref, *refs):
    sort_rows(me_ref[0], refs[:-1], refs[-1])


def sort(me, xs):
    block_rows, depth = xs[0].shape
    return pl.pallas_call(
        sort_kernel,
        in_specs=[SMEM] + [VMEM] * len(xs),
        out_specs=VMEM,
        out_shape=jax.ShapeDtypeStruct((block_rows * len(xs), depth), xs[0].dtype),
        compiler_params=pltpu.CompilerParams(vmem_limit_bytes=12 * MIB),
        cost_estimate=pl.CostEstimate(flops=10**10, bytes_accessed=0, transcendentals=0),
        name="sort",
    )(me, *[pltpu.with_memory_space_constraint(x, pltpu.HBM) for x in xs])


def up_gate_kernel(me_ref, *refs, blocks, first):
    x_refs, (g_ref, u_ref, send_ref, keep_ref, *scratch) = refs[:blocks], refs[blocks:]
    if scratch:
        sort_rows(me_ref[0], x_refs, scratch[0])
    x = (scratch or x_refs)[0][...]
    half = x.shape[0] // 2
    if x.shape[0] < 128:
        x = jnp.concatenate([x, x], axis=0)
    share = send_ref.shape[2]
    width = width_of(share)
    for j in range(share // width):
        cols = slice(j * width, (j + 1) * width)
        taken = slice(first + j * width, first + (j + 1) * width)
        for i, w_ref in enumerate((g_ref, u_ref)):
            y = jnp.dot(x, w_ref[:, taken], preferred_element_type=jnp.float32)
            send_ref[i, :, cols] = y[:half].astype(send_ref.dtype)
            keep_ref[i, :, cols] = y[half : 2 * half]


def up_gate(me, xs, gate, up, ordered, piece, pieces):
    depth, hidden = gate.shape[0], gate.shape[1] // pieces
    rows = xs[0].shape[0] * len(xs)
    return pl.pallas_call(
        functools.partial(up_gate_kernel, blocks=len(xs), first=piece * hidden),
        in_specs=[SMEM] + [VMEM] * (len(xs) + 2),
        out_specs=[VMEM] * 2,
        out_shape=[
            jax.ShapeDtypeStruct((2, rows // 2, hidden), jnp.bfloat16),
            jax.ShapeDtypeStruct((2, rows // 2, hidden), jnp.float32),
        ],
        scratch_shapes=[] if ordered else [pltpu.VMEM((rows, depth), jnp.bfloat16)],
        compiler_params=pltpu.CompilerParams(vmem_limit_bytes=12 * MIB),
        cost_estimate=pl.CostEstimate(
            flops=4 * rows * depth * hidden, bytes_accessed=4 * depth * hidden, transcendentals=0
        ),
        name="up_gate",
    )(me, *xs, held(gate), held(up))


def down_kernel(me_ref, h0, h2, h1, h3, w_ref, *refs, blocks):
    outs, adds = refs[-blocks:], refs[:-blocks]
    me = me_ref[0]
    h = jnp.concatenate([h0[...], h2[...], h1[...], h3[...]], axis=0)
    if h.shape[0] < 128:
        h = jnp.concatenate([h, h], axis=0)
    part = outs[0].shape[0] // len(ORDER)
    depth = w_ref.shape[1]
    width = 256 if depth % 256 == 0 else depth
    for c in range(depth // width):
        cols = slice(c * width, (c + 1) * width)
        y = jnp.dot(h, w_ref[:, cols], preferred_element_type=jnp.float32)
        for i, r in enumerate((0, 2, 1, 3)):
            at = pl.multiple_of((me ^ r) * part, part)
            for b, out in enumerate(outs):
                first = (i * len(outs) + b) * part
                value = y[first : first + part]
                if adds:
                    value += adds[b][pl.ds(at, part), cols].astype(jnp.float32)
                out[pl.ds(at, part), cols] = value.astype(out.dtype)


def down(me, hs, weight, block_rows, kinds, adds):
    hidden, depth = weight.shape
    rows = block_rows * len(kinds)
    return pl.pallas_call(
        functools.partial(down_kernel, blocks=len(kinds)),
        in_specs=[SMEM] + [VMEM] * (5 + len(adds)),
        out_specs=[VMEM] * len(kinds),
        out_shape=[jax.ShapeDtypeStruct((block_rows, depth), kind) for kind in kinds],
        compiler_params=pltpu.CompilerParams(vmem_limit_bytes=12 * MIB),
        cost_estimate=pl.CostEstimate(
            flops=2 * rows * depth * hidden, bytes_accessed=2 * depth * hidden, transcendentals=0
        ),
        name="down",
    )(me, *hs, held(weight), *adds)


def steps(tokens, gate_weight, up_weight, down_weight):
    grid_size = lax.axis_size("grid")
    block_rows = tokens.shape[0]
    me = lax.axis_index("depth").astype(jnp.int32).reshape(1)
    per = grid_size // sum(map(len, CHUNKS))
    chunks = [[s for q in chunk for s in range(q * per, (q + 1) * per)] for chunk in CHUNKS]
    blocks = {0: tokens}
    for chunk in chunks:
        for s in chunk:
            if s:
                blocks[s] = flip(tokens, "grid", s)
    total = None
    arrived, relayed = [], {}
    for number, chunk in enumerate(chunks):
        xs = [blocks[s] for s in chunk]
        if number == 0:
            xs = [sort(me, xs)]
        pieces = SPLIT.get(number, 1) if gate_weight.shape[1] % 256 == 0 else 1
        sums = []
        for piece in range(pieces):
            send, keep = up_gate(me, xs, gate_weight, up_weight, number == 0, piece, pieces)
            part = keep.shape[1] // 2
            recv = flip(send, "depth", 1)
            across = (keep[:, :part] + recv[:, :part].astype(jnp.float32)).astype(jnp.bfloat16)
            crossed = flip(across, "depth", 2)
            sums.append((keep, recv, crossed))
        mine = []
        for keep, recv, crossed in sums:
            both = keep[:, part:] + recv[:, part:].astype(jnp.float32) + crossed.astype(jnp.float32)
            mine.append((jax.nn.silu(both[0]) * both[1]).astype(jnp.bfloat16))
        mine = jnp.concatenate(mine, axis=1)
        other = flip(mine, "depth", 2)
        mine_passed = flip(mine, "depth", 1)
        other_passed = flip(other, "depth", 1)
        kinds = [jnp.bfloat16 if s else jnp.float32 for s in chunk]
        adds = [relayed[s] for s in chunk if s in relayed]
        outs = down(me, (mine, other, mine_passed, other_passed), down_weight, block_rows, kinds, adds)
        for s, out in zip(chunk, outs):
            if s == 0:
                total = out
            else:
                if number == FAR:
                    relayed[s ^ per] = flip(out, "grid", per)
                else:
                    arrived.append(flip(out, "grid", s))
    for value in arrived:
        total = total + value.astype(jnp.float32)
    return total.astype(jnp.bfloat16)


def solution(mesh):
    placed = (
        P(("groups", "grid"), "depth"),
        P("depth", "grid"),
        P("depth", "grid"),
        P("grid", "depth"),
    )
    return jax.shard_map(
        steps, mesh=mesh, in_specs=placed, out_specs=P(("groups", "grid"), "depth"), check_vma=False
    )
```
